128 devices in a mesh: dp: 1, sp: 64 (over z, y, x), tp: 2 (over core).
Axes of the slice: x: 4, y: 4, z: 4, core: 2. Of those that a mesh axis runs over, the one named last changes fastest.
Arguments:
- hidden_in: bfloat16 [8192, 1536], P(('dp', 'sp', 'tp'))
- segment_ids: int32 [8192], P(('dp', 'sp', 'tp'))
- positions: int32 [8192], P(('dp', 'sp', 'tp'))
- attn_gain: bfloat16 [8, 1536], replicated
- w_q: bfloat16 [8, 1536, 1536], P(None, None, 'tp')
- w_k: bfloat16 [8, 1536, 256], P(None, None, 'tp')
- w_v: bfloat16 [8, 1536, 256], P(None, None, 'tp')
- w_o: bfloat16 [8, 1536, 1536], P(None, 'tp')
- mlp_gain: bfloat16 [8, 1536], replicated
- w_gate: bfloat16 [8, 1536, 8960], P(None, None, 'tp')
- w_up: bfloat16 [8, 1536, 8960], P(None, None, 'tp')
- w_down: bfloat16 [8, 8960, 1536], P(None, 'tp')
Outputs:
- output 1: bfloat16 [8192, 1536], P(('dp', 'sp', 'tp'))
- output 2: bfloat16 [8, 8192, 2, 128], P(None, ('dp', 'sp'), 'tp')
- output 3: bfloat16 [8, 8192, 2, 128], P(None, ('dp', 'sp'), 'tp')
All inputs are finite; a program needn't handle non-finite values.
Results may differ from the reference program's by a relative error of at most 0.02.
Values are sent between devices in bfloat16 or wider.
A program may use at most 1.5 GiB of HBM per device.

```python
import math
import jax
import jax.numpy as jnp
from jax import lax

TOKENS = 8192
MODEL_DIM = 1536
HEADS = 12
KV_HEADS = 2
HEAD_DIM = 128
FFN_DIM = 8960
LAYERS = 8
SEGMENTS = 4

GROUP = HEADS // KV_HEADS
Q_BLOCK = math.gcd(TOKENS, 32)
ROPE_BASE = 1e4
NORM_EPS = 1e-5
SCORE_SCALE = HEAD_DIM ** -0.5


def setup_inputs(seed: int = 0, part: int = 0) -> dict:
    part_key = jax.random.fold_in(jax.random.key(seed), part)
    act_keys = jax.random.split(part_key, 6)
    base_noise = jax.random.normal(act_keys[0], (TOKENS, MODEL_DIM), jnp.float32)
    cycles = jax.random.uniform(act_keys[1], (MODEL_DIM,), jnp.float32, 0.5, 3.0)
    phases = jax.random.uniform(act_keys[2], (MODEL_DIM,), jnp.float32, 0.0, 6.2832)
    time_ramp = jnp.arange(TOKENS, dtype=jnp.float32) / TOKENS
    drift_part = jnp.cos(6.2832 * time_ramp[:, None] * cycles[None, :] + phases[None, :])
    hidden_in = (0.6 * base_noise + 1.2 * drift_part).astype(jnp.bfloat16)
    cut_points = jax.random.permutation(act_keys[3], TOKENS - 1)[: SEGMENTS - 1] + 1
    seg_marks = jnp.zeros((TOKENS,), jnp.int32).at[cut_points].set(1)
    segment_ids = jnp.cumsum(seg_marks).astype(jnp.int32)
    pos_steps = jax.random.randint(act_keys[4], (TOKENS,), 1, 3)
    pos_start = jax.random.randint(act_keys[5], (), 0, 64)
    positions = (jnp.cumsum(pos_steps) + pos_start).astype(jnp.int32)
    w_keys = jax.random.split(jax.random.key(seed + 1), 9)

    def normal_w(key_w, shape_w, scale_w):
        return (jax.random.normal(key_w, shape_w, jnp.float32) * scale_w).astype(jnp.bfloat16)

    def gain_w(key_w):
        return (1.0 + 0.3 * jax.random.normal(key_w, (LAYERS, MODEL_DIM), jnp.float32)).astype(jnp.bfloat16)

    dim_scale = MODEL_DIM ** -0.5
    return {
        'hidden_in': hidden_in,
        'segment_ids': segment_ids,
        'positions': positions,
        'attn_gain': gain_w(w_keys[0]),
        'w_q': normal_w(w_keys[1], (LAYERS, MODEL_DIM, HEADS * HEAD_DIM), 1.4 * dim_scale),
        'w_k': normal_w(w_keys[2], (LAYERS, MODEL_DIM, KV_HEADS * HEAD_DIM), 1.4 * dim_scale),
        'w_v': normal_w(w_keys[3], (LAYERS, MODEL_DIM, KV_HEADS * HEAD_DIM), dim_scale),
        'w_o': normal_w(w_keys[4], (LAYERS, HEADS * HEAD_DIM, MODEL_DIM), 0.7 * (HEADS * HEAD_DIM) ** -0.5),
        'mlp_gain': gain_w(w_keys[5]),
        'w_gate': normal_w(w_keys[6], (LAYERS, MODEL_DIM, FFN_DIM), dim_scale),
        'w_up': normal_w(w_keys[7], (LAYERS, MODEL_DIM, FFN_DIM), dim_scale),
        'w_down': normal_w(w_keys[8], (LAYERS, FFN_DIM, MODEL_DIM), 0.7 * FFN_DIM ** -0.5),
    }


def rms_norm(hidden, gain_vec):
    hidden32 = hidden.astype(jnp.float32)
    inv_rms = lax.rsqrt(jnp.mean(hidden32 * hidden32, axis=-1, keepdims=True) + NORM_EPS)
    return (hidden32 * inv_rms * gain_vec.astype(jnp.float32)).astype(jnp.bfloat16)


def rotary(rot_in, positions):
    half_dim = HEAD_DIM // 2
    inv_freq = ROPE_BASE ** (-jnp.arange(half_dim, dtype=jnp.float32) / half_dim)
    angles = positions.astype(jnp.float32)[..., None] * inv_freq
    cos_val = jnp.cos(angles)[..., None, :]
    sin_val = jnp.sin(angles)[..., None, :]
    first_half = rot_in[..., :half_dim]
    second_half = rot_in[..., half_dim:]
    return jnp.concatenate([first_half * cos_val - second_half * sin_val, second_half * cos_val + first_half * sin_val], axis=-1)


def attention(q_rot, k_rot, v_val, segment_ids):
    n_blocks = TOKENS // Q_BLOCK
    key_index = jnp.arange(TOKENS)
    k_wide = k_rot.astype(jnp.float32)
    v_wide = v_val.astype(jnp.float32)

    def one_block(block_in):
        q_blk, idx_blk, seg_blk = block_in
        scores = jnp.einsum('qkgd,skd->kgqs', q_blk.astype(jnp.float32), k_wide) * SCORE_SCALE
        allowed = (idx_blk[:, None] >= key_index[None, :]) & (seg_blk[:, None] == segment_ids[None, :])
        probs = jax.nn.softmax(jnp.where(allowed, scores, -1e30), axis=-1).astype(jnp.bfloat16)
        return jnp.einsum('kgqs,skd->qkgd', probs.astype(jnp.float32), v_wide).astype(jnp.bfloat16)

    blocks = (q_rot.reshape(n_blocks, Q_BLOCK, KV_HEADS, GROUP, HEAD_DIM),
              key_index.reshape(n_blocks, Q_BLOCK), segment_ids.reshape(n_blocks, Q_BLOCK))
    return lax.map(one_block, blocks).reshape(TOKENS, HEADS * HEAD_DIM)


def reference(hidden_in, segment_ids, positions, attn_gain, w_q, w_k, w_v, w_o, mlp_gain, w_gate, w_up, w_down):
    def layer_step(hidden, layer_w):
        gain_attn, wq_l, wk_l, wv_l, wo_l, gain_mlp, wg_l, wu_l, wd_l = layer_w
        normed = rms_norm(hidden, gain_attn)
        q_lin = jnp.dot(normed, wq_l, preferred_element_type=jnp.float32).reshape(TOKENS, HEADS, HEAD_DIM)
        k_lin = jnp.dot(normed, wk_l, preferred_element_type=jnp.float32).reshape(TOKENS, KV_HEADS, HEAD_DIM)
        v_val = jnp.dot(normed, wv_l, preferred_element_type=jnp.float32).astype(jnp.bfloat16).reshape(TOKENS, KV_HEADS, HEAD_DIM)
        q_rot = rotary(q_lin, positions).astype(jnp.bfloat16).reshape(TOKENS, KV_HEADS, GROUP, HEAD_DIM)
        k_rot = rotary(k_lin, positions).astype(jnp.bfloat16)
        att_out = attention(q_rot, k_rot, v_val, segment_ids)
        proj_out = jnp.dot(att_out, wo_l, preferred_element_type=jnp.float32).astype(jnp.bfloat16)
        hidden_mid = (hidden.astype(jnp.float32) + proj_out.astype(jnp.float32)).astype(jnp.bfloat16)
        normed_mlp = rms_norm(hidden_mid, gain_mlp)
        gate_lin = jnp.dot(normed_mlp, wg_l, preferred_element_type=jnp.float32)
        up_lin = jnp.dot(normed_mlp, wu_l, preferred_element_type=jnp.float32)
        act_vals = (jax.nn.silu(gate_lin) * up_lin).astype(jnp.bfloat16)
        down_out = jnp.dot(act_vals, wd_l, preferred_element_type=jnp.float32).astype(jnp.bfloat16)
        hidden_new = (hidden_mid.astype(jnp.float32) + down_out.astype(jnp.float32)).astype(jnp.bfloat16)
        return hidden_new, (k_rot, v_val)

    hidden_out, caches = lax.scan(layer_step, hidden_in, (attn_gain, w_q, w_k, w_v, w_o, mlp_gain, w_gate, w_up, w_down))
    return hidden_out, caches[0], caches[1]
```

```python
import math
import jax
import jax.numpy as jnp
from jax import lax
from jax.experimental import pallas as pl
from jax.experimental.pallas import tpu as pltpu
from jax.sharding import PartitionSpec as P

HEAD_DIM = 128
ROPE_BASE = 1e4
NORM_EPS = 1e-5
SCORE_SCALE = HEAD_DIM ** -0.5
EXP_SCALE = SCORE_SCALE * math.log2(math.e)
BIG = 1e30
MESH = pl.DeviceIdType.MESH
F32 = jnp.float32
BF16 = jnp.bfloat16

PART_ROWS = (48, 48, 32)
PART_OFF = (0, 48, 96)
PART_STRIDES = ((1, 4, 16), (4, 16, 1), (16, 1, 4))
N_SEM = 23


def rms_rows(x_val, gain_row):
    x32 = x_val.astype(F32)
    inv_rms = lax.rsqrt(jnp.mean(x32 * x32, axis=-1, keepdims=True) + NORM_EPS)
    return (x32 * inv_rms * gain_row).astype(BF16)


def stack_kernel(n_layers, rows, half_rows, hid_ref, aux_ref, ga_ref, gm_ref, wq_h, wk_h, wv_h, wo_h, wg_h, wu_h, wd_h,
                 hid_out, k_out, v_out,
                 x_buf, aux_buf, cnt_buf, wqkv, wo, wg, wu, wd, kv0, kv1, kv2, ext0, ext1, ext2, q_t, mask_add,
                 m_s, l_s, acc_s, n_s, o_s, act_s, kst, vst, snd_a, rcv_a, snd_b, rcv_b,
                 ini_ss, ini_rs, cnt_ss, cnt_rs, w_sem, g_ss, g_rs, x_ss, x_rs, c_sem):
    sp = lax.axis_index('sp')
    tp = lax.axis_index('tp')
    kvs = (kv0, kv1, kv2)
    exts = (ext0, ext1, ext2)
    n_q = wq_h.shape[2]
    n_heads = n_q // HEAD_DIM
    d_model = hid_ref.shape[1]
    ffn = wg_h.shape[2]

    def coord(stride):
        return (sp // stride) % 4

    def neighbour(stride, delta):
        here = coord(stride)
        return sp + ((here + delta) % 4 - here) * stride

    def remote(src, dst, ss, rs, sp_to, tp_to):
        return pltpu.make_async_remote_copy(src_ref=src, dst_ref=dst, send_sem=ss, recv_sem=rs,
                                            device_id={'sp': sp_to, 'tp': tp_to}, device_id_type=MESH)

    n_split = 4
    gr = d_model // n_split
    dr = ffn // n_split

    def qkv_copies(layer):
        nk = wk_h.shape[2]
        return [pltpu.make_async_copy(wq_h.at[layer], wqkv.at[:, 0:n_q], w_sem.at[0]),
                pltpu.make_async_copy(wk_h.at[layer], wqkv.at[:, n_q:n_q + nk], w_sem.at[1]),
                pltpu.make_async_copy(wv_h.at[layer], wqkv.at[:, n_q + nk:n_q + 2 * nk], w_sem.at[2])]

    def wo_copies(layer):
        return [pltpu.make_async_copy(wo_h.at[layer], wo, w_sem.at[3])]

    def gu_copies(layer):
        out = []
        for c in range(n_split):
            r = pl.ds(c * gr, gr)
            out.append(pltpu.make_async_copy(wg_h.at[layer, r], wg.at[r], w_sem.at[4 + c]))
            out.append(pltpu.make_async_copy(wu_h.at[layer, r], wu.at[r], w_sem.at[4 + n_split + c]))
        return out

    def down_copies(layer):
        out = []
        for c in range(n_split):
            r = pl.ds(c * dr, dr)
            out.append(pltpu.make_async_copy(wd_h.at[layer, r], wd.at[r], w_sem.at[4 + 2 * n_split + c]))
        return out

    def start_all(copies):
        for c in copies:
            c.start()

    def wait_all(copies):
        for c in copies:
            c.wait()

    start_all(qkv_copies(0))
    start_all(wo_copies(0))
    start_all(gu_copies(0))
    start_all(down_copies(0))

    barrier = pltpu.get_barrier_semaphore()
    for stride in (1, 4, 16):
        for delta in (1, 2, 3):
            pl.semaphore_signal(barrier, inc=1, device_id={'sp': neighbour(stride, delta), 'tp': tp}, device_id_type=MESH)
    pl.semaphore_signal(barrier, inc=1, device_id={'sp': sp, 'tp': 1 - tp}, device_id_type=MESH)
    pl.semaphore_wait(barrier, 10)

    mine = pl.ds(pl.multiple_of(tp * half_rows, half_rows), half_rows)
    theirs = pl.ds(pl.multiple_of((1 - tp) * half_rows, half_rows), half_rows)
    swaps = [remote(hid_ref, x_buf.at[mine], ini_ss.at[0], ini_rs.at[0], sp, 1 - tp),
             remote(aux_ref, aux_buf.at[:, mine], ini_ss.at[1], ini_rs.at[1], sp, 1 - tp)]
    start_all(swaps)
    x_buf[mine, :] = hid_ref[...]
    for a in range(3):
        aux_buf[a, mine, :] = aux_ref[a]
    for s in swaps:
        s.wait_send()
    remote(hid_ref, x_buf.at[theirs], ini_ss.at[0], ini_rs.at[0], sp, 1 - tp).wait_recv()
    remote(aux_ref, aux_buf.at[:, theirs], ini_ss.at[1], ini_rs.at[1], sp, 1 - tp).wait_recv()

    seg_col = aux_buf[2]
    lane_f = lax.broadcasted_iota(jnp.int32, (rows, 128), 1).astype(F32)
    below = jnp.sum(jnp.where(seg_col < lane_f, 1.0, 0.0), axis=0, keepdims=True)
    upto = jnp.sum(jnp.where(seg_col < lane_f + 1.0, 1.0, 0.0), axis=0, keepdims=True)
    mx, my, mz = coord(1), coord(4), coord(16)
    cnt_buf[mz, my, mx] = jnp.concatenate([jnp.broadcast_to(below, (8, 128)), jnp.broadcast_to(upto, (8, 128))], axis=0)
    for phase, stride in enumerate((1, 4, 16)):
        def block(cz, cy, cx):
            return (cnt_buf.at[cz, cy, cx], cnt_buf.at[cz, cy], cnt_buf.at[cz])[phase]
        for delta in (1, 2, 3):
            b = block(mz, my, mx)
            i = phase * 3 + delta - 1
            remote(b, b, cnt_ss.at[i], cnt_rs.at[i], neighbour(stride, delta), tp).start()
        for delta in (1, 2, 3):
            i = phase * 3 + delta - 1
            frm = [mz, my, mx]
            frm[2 - phase] = (frm[2 - phase] - delta) % 4
            b = block(*frm)
            c = remote(b, b, cnt_ss.at[i], cnt_rs.at[i], neighbour(stride, delta), tp)
            c.wait_send()
            c.wait_recv()
    total = jnp.sum(cnt_buf[...].reshape(64, 16, 128), axis=0)
    seg_lo = total[0:1, :]
    seg_hi = total[8:9, :]

    for p in range(3):
        s1, s2, s3 = PART_STRIDES[p]
        pr = PART_ROWS[p]
        row_i = lax.broadcasted_iota(jnp.int32, (pr, 128), 0)
        lane_i = lax.broadcasted_iota(jnp.int32, (pr, 128), 1)

        def fill(b, carry, p=p, s1=s1, s2=s2, s3=s3, pr=pr, row_i=row_i, lane_i=lane_i):
            c3 = b // 16
            c2 = (b // 4) % 4
            c1 = b % 4
            blk = c3 * s3 + c2 * s2 + c1 * s1
            idx = (row_i + (blk * rows + PART_OFF[p])).astype(F32)
            one_hot = jnp.where(idx >= seg_lo, 1.0, 0.0) * jnp.where(idx < seg_hi, 1.0, 0.0)
            late = jnp.where(row_i * 0 + blk >= sp, 1.0, 0.0)
            val = jnp.where(lane_i < 4, one_hot, jnp.where(lane_i == 4, late, 0.0))
            exts[p][c3, c2, c1] = val.astype(BF16)
            return carry
        lax.fori_loop(0, 64, fill, 0)

    seg_row = jnp.transpose(seg_col)
    row_i = lax.broadcasted_iota(jnp.int32, (rows, 128), 0)
    col_i = lax.broadcasted_iota(jnp.int32, (rows, 128), 1)
    q_side = jnp.where(row_i < 4, jnp.where(seg_row == row_i.astype(F32), 0.0, -BIG), jnp.where(row_i == 4, -BIG, 0.0)).astype(BF16)
    for h in range(n_heads):
        q_t[128:256, h * 128:(h + 1) * 128] = q_side
    mask_add[...] = jnp.where(row_i <= col_i, jnp.where(seg_col == seg_row, 0.0, -BIG), -BIG)

    def soft_step(keys, vals, cols, add, first):
        n_c = cols.stop - cols.start
        q_rows = slice(0, keys.shape[1])
        s = jnp.dot(keys, q_t[q_rows, cols], preferred_element_type=F32)
        if add is not None:
            s = s + add
        top = jnp.max(s, axis=0, keepdims=True)
        if first:
            m_new = top
        else:
            m_old = m_s[0:1, cols]
            m_new = jnp.maximum(m_old, top)
        e = jnp.exp2((s - m_new) * EXP_SCALE)
        e_sum = jnp.sum(e, axis=0, keepdims=True)
        pv = lax.dot_general(vals, e.astype(BF16), (((0,), (0,)), ((), ())), preferred_element_type=F32)
        if first:
            l_new = e_sum
            acc_s[:, cols] = pv
        else:
            alpha = jnp.exp2((m_old - m_new) * EXP_SCALE)
            l_new = l_s[0:1, cols] * alpha + e_sum
            acc_s[:, cols] = acc_s[:, cols] * alpha + pv
        m_s[:, cols] = jnp.broadcast_to(m_new, (8, n_c))
        l_s[:, cols] = jnp.broadcast_to(l_new, (8, n_c))

    col_tiles = [slice(c, c + 256) for c in range(0, n_q, 256)]

    def plane_step(p, par, c3):
        n_k = 16 * PART_ROWS[p]
        kv = kvs[p][par, c3].reshape(n_k, 256)
        keys = jnp.concatenate([kv[:, 0:128], exts[p][c3].reshape(n_k, 128)], axis=1)
        for cols in col_tiles:
            soft_step(keys, kv[:, 128:256], cols, None, False)

    def layer_step(layer, carry):
        par = layer % 2
        has_next = layer + 1 < n_layers

        def send(p, i, ref, stride, delta):
            remote(ref, ref, g_ss.at[p, i], g_rs.at[par, p, i], neighbour(stride, delta), tp).start()

        def got(p, i, ref):
            remote(ref, ref, g_ss.at[p, i], g_rs.at[par, p, i], sp, 1 - tp).wait_recv()

        def sent(p, i, ref):
            remote(ref, ref, g_ss.at[p, i], g_rs.at[par, p, i], sp, 1 - tp).wait_send()

        coords = [tuple(coord(s) for s in PART_STRIDES[p]) for p in range(3)]

        n_s[...] = rms_rows(x_buf[...], ga_ref[layer])
        wait_all(qkv_copies(layer))
        cos_t = aux_buf[0]
        sin_t = aux_buf[1]

        def rope(v):
            return (v * cos_t + pltpu.roll(v, HEAD_DIM // 2, 1) * sin_t).astype(BF16)

        kv_lin = jnp.dot(n_s[...], wqkv[:, n_q:], preferred_element_type=F32)
        k_rot = rope(kv_lin[:, 0:128])
        v_val = kv_lin[:, 128:256].astype(BF16)
        kst[...] = k_rot
        vst[...] = v_val
        kv_val = jnp.concatenate([k_rot, v_val], axis=1)
        for p in range(3):
            m1, m2, m3 = coords[p]
            kvs[p][par, m3, m2, m1] = kv_val[PART_OFF[p]:PART_OFF[p] + PART_ROWS[p], :]
        cache = [pltpu.make_async_copy(kst, k_out.at[layer], c_sem.at[0]),
                 pltpu.make_async_copy(vst, v_out.at[layer], c_sem.at[1])]
        start_all(cache)
        for p in range(3):
            m1, m2, m3 = coords[p]
            own = kvs[p].at[par, m3, m2, m1]
            for i, delta in enumerate((1, 3, 2)):
                send(p, i, own, PART_STRIDES[p][0], delta)
        q_lin = jnp.dot(n_s[...], wqkv[:, 0:n_q], preferred_element_type=F32)
        for h in range(n_heads):
            q_h = rope(q_lin[:, h * 128:(h + 1) * 128])
            q_t[0:128, h * 128:(h + 1) * 128] = jnp.transpose(q_h)

        @pl.when(has_next)
        def _():
            start_all(qkv_copies(layer + 1))

        mask2 = jnp.concatenate([mask_add[...], mask_add[...]], axis=1)
        for cols in col_tiles:
            soft_step(kst[...], vst[...], cols, mask2, True)

        for p in range(3):
            m1, m2, m3 = coords[p]
            s1, s2, s3 = PART_STRIDES[p]
            for i, delta in enumerate((1, 3, 2)):
                got(p, i, kvs[p].at[par, m3, m2, (m1 - delta) % 4])
            row = kvs[p].at[par, m3, m2]
            send(p, 3, row, s2, 1)
            send(p, 4, row, s2, 3)
            send(p, 7, row, s3, 1)
            send(p, 8, row, s3, 3)

        def pass_on3(p, r, c2):
            m1, m2, m3 = coords[p]
            s3 = PART_STRIDES[p][2]
            lo = (m3 - 1) % 4
            hi = (m3 + 1) % 4
            got(p, 7 + 4 * r, kvs[p].at[par, lo, c2])
            send(p, 9 + 4 * r, kvs[p].at[par, lo, c2, 0:2], s3, 1)
            got(p, 8 + 4 * r, kvs[p].at[par, hi, c2])
            send(p, 10 + 4 * r, kvs[p].at[par, hi, c2, 2:4], s3, 3)

        for p in range(3):
            m1, m2, m3 = coords[p]
            s1, s2, s3 = PART_STRIDES[p]
            lo = (m2 - 1) % 4
            hi = (m2 + 1) % 4
            got(p, 3, kvs[p].at[par, m3, lo])
            send(p, 5, kvs[p].at[par, m3, lo, 0:2], s2, 1)
            send(p, 11, kvs[p].at[par, m3, lo], s3, 1)
            send(p, 12, kvs[p].at[par, m3, lo], s3, 3)
            got(p, 4, kvs[p].at[par, m3, hi])
            send(p, 6, kvs[p].at[par, m3, hi, 2:4], s2, 3)
            send(p, 15, kvs[p].at[par, m3, hi], s3, 1)
            send(p, 16, kvs[p].at[par, m3, hi], s3, 3)
        for p in range(3):
            pass_on3(p, 0, coords[p][1])
        for p in range(3):
            m1, m2, m3 = coords[p]
            s1, s2, s3 = PART_STRIDES[p]
            far = (m2 + 2) % 4
            got(p, 5, kvs[p].at[par, m3, far, 0:2])
            got(p, 6, kvs[p].at[par, m3, far, 2:4])
            send(p, 19, kvs[p].at[par, m3, far], s3, 1)
            send(p, 20, kvs[p].at[par, m3, far], s3, 3)
        for p in range(3):
            plane_step(p, par, coords[p][2])
        for r, off in ((1, 3), (2, 1), (3, 2)):
            for p in range(3):
                pass_on3(p, r, (coords[p][1] + off) % 4)
        for p in range(3):
            plane_step(p, par, (coords[p][2] + 3) % 4)
        for p in range(3):
            plane_step(p, par, (coords[p][2] + 1) % 4)
        for p in range(3):
            m1, m2, m3 = coords[p]
            far = (m3 + 2) % 4
            for r, off in ((0, 0), (1, 3), (2, 1), (3, 2)):
                c2 = (m2 + off) % 4
                got(p, 9 + 4 * r, kvs[p].at[par, far, c2, 0:2])
                got(p, 10 + 4 * r, kvs[p].at[par, far, c2, 2:4])
            plane_step(p, par, far)

        for h in range(n_heads):
            cols = slice(h * 128, (h + 1) * 128)
            o_t = acc_s[:, cols] * (1.0 / l_s[0:1, cols])
            o_s[:, cols] = jnp.transpose(o_t.astype(BF16))
        wait_all(wo_copies(layer))
        n_t = snd_a.shape[0]
        tw = snd_a.shape[2]
        swap_a = [remote(snd_a.at[t], rcv_a.at[t], x_ss.at[0, t], x_rs.at[0, t], sp, 1 - tp) for t in range(n_t)]
        swap_b = [remote(snd_b.at[t], rcv_b.at[t], x_ss.at[1, t], x_rs.at[1, t], sp, 1 - tp) for t in range(n_t)]
        for t in range(n_t):
            part = jnp.dot(o_s[...], wo[:, t * tw:(t + 1) * tw], preferred_element_type=F32)
            snd_a[t] = part.astype(BF16)
            swap_a[t].start()

        for p in range(3):
            m1, m2, m3 = coords[p]
            for i in range(3):
                sent(p, i, kvs[p].at[par, m3, m2, m1])
            for i in (3, 4):
                sent(p, i, kvs[p].at[par, m3, m2])
            for i in (5, 6):
                sent(p, i, kvs[p].at[par, m3, m2, 0:2])
            for r in range(4):
                for i in (7, 8):
                    sent(p, i + 4 * r, kvs[p].at[par, m3, m2])
                for i in (9, 10):
                    sent(p, i + 4 * r, kvs[p].at[par, m3, m2, 0:2])

        @pl.when(has_next)
        def _():
            start_all(wo_copies(layer + 1))

        for t in range(n_t):
            swap_a[t].wait()
            cols = slice(t * tw, (t + 1) * tw)
            res = (snd_a[t].astype(F32) + rcv_a[t].astype(F32)).astype(BF16)
            x_buf[:, cols] = (x_buf[:, cols].astype(F32) + res.astype(F32)).astype(BF16)

        n_s[...] = rms_rows(x_buf[...], gm_ref[layer])
        wait_all(gu_copies(layer))

        def gate_up(cols):
            gate = jnp.dot(n_s[...], wg[:, cols], preferred_element_type=F32)
            up = jnp.dot(n_s[...], wu[:, cols], preferred_element_type=F32)
            act_s[:, cols] = (gate * jax.nn.sigmoid(gate) * up).astype(BF16)

        gt = 1024

        def gate_up_tile(t, c):
            gate_up(pl.ds(pl.multiple_of(t * gt, gt), gt))
            return c
        n_full = ffn // gt
        lax.fori_loop(0, n_full, gate_up_tile, 0)
        if ffn % gt:
            gate_up(slice(n_full * gt, ffn))

        @pl.when(has_next)
        def _():
            start_all(gu_copies(layer + 1))

        wait_all(down_copies(layer))
        for t in range(n_t):
            part = jnp.dot(act_s[...], wd[:, t * tw:(t + 1) * tw], preferred_element_type=F32)
            snd_b[t] = part.astype(BF16)
            swap_b[t].start()

        @pl.when(has_next)
        def _():
            start_all(down_copies(layer + 1))

        wait_all(cache)
        for t in range(n_t):
            swap_b[t].wait()
            cols = slice(t * tw, (t + 1) * tw)
            res = (snd_b[t].astype(F32) + rcv_b[t].astype(F32)).astype(BF16)
            x_buf[:, cols] = (x_buf[:, cols].astype(F32) + res.astype(F32)).astype(BF16)
        return carry

    lax.fori_loop(0, n_layers, layer_step, 0)
    hid_out[...] = x_buf[mine, :]


def solution(mesh):
    tok_spec = P(('dp', 'sp', 'tp'))
    col_spec = P(None, None, 'tp')
    row_spec = P(None, 'tp', None)
    cache_spec = P(None, ('dp', 'sp'), 'tp', None)

    def device_fn(hidden_in, segment_ids, positions, attn_gain, w_q, w_k, w_v, w_o, mlp_gain, w_gate, w_up, w_down):
        half_rows, d_model = hidden_in.shape
        rows = 2 * half_rows
        n_layers, _, n_q = w_q.shape
        ffn = w_gate.shape[2]
        half_dim = HEAD_DIM // 2
        inv_freq = ROPE_BASE ** (-jnp.arange(half_dim, dtype=F32) / half_dim)
        angles = positions.astype(F32)[:, None] * inv_freq
        cos_val = jnp.cos(angles)
        sin_val = jnp.sin(angles)
        aux = jnp.stack([jnp.concatenate([cos_val, cos_val], axis=1), jnp.concatenate([-sin_val, sin_val], axis=1),
                         jnp.broadcast_to(segment_ids.astype(F32)[:, None], (half_rows, HEAD_DIM))])
        vm = pl.BlockSpec(memory_space=pltpu.VMEM)
        anyspec = pl.BlockSpec(memory_space=pl.ANY)
        n_t, tw = 3, d_model // 3
        dma = pltpu.SemaphoreType.DMA
        body = lambda *refs: stack_kernel(n_layers, rows, half_rows, *refs)
        hid, k_c, v_c = pl.pallas_call(
            body,
            out_shape=(jax.ShapeDtypeStruct((half_rows, d_model), BF16),
                       jax.ShapeDtypeStruct((n_layers, rows, HEAD_DIM), BF16),
                       jax.ShapeDtypeStruct((n_layers, rows, HEAD_DIM), BF16)),
            in_specs=[vm, vm, vm, vm] + [anyspec] * 7,
            out_specs=(vm, anyspec, anyspec),
            scratch_shapes=[
                pltpu.VMEM((rows, d_model), BF16),
                pltpu.VMEM((3, rows, 128), F32),
                pltpu.VMEM((4, 4, 4, 16, 128), F32),
                pltpu.VMEM((d_model, n_q + 2 * HEAD_DIM), BF16),
                pltpu.VMEM((n_q, d_model), BF16),
                pltpu.VMEM((d_model, ffn), BF16),
                pltpu.VMEM((d_model, ffn), BF16),
                pltpu.VMEM((ffn, d_model), BF16),
                pltpu.VMEM((2, 4, 4, 4, PART_ROWS[0], 256), BF16),
                pltpu.VMEM((2, 4, 4, 4, PART_ROWS[1], 256), BF16),
                pltpu.VMEM((2, 4, 4, 4, PART_ROWS[2], 256), BF16),
                pltpu.VMEM((4, 4, 4, PART_ROWS[0], 128), BF16),
                pltpu.VMEM((4, 4, 4, PART_ROWS[1], 128), BF16),
                pltpu.VMEM((4, 4, 4, PART_ROWS[2], 128), BF16),
                pltpu.VMEM((256, n_q), BF16),
                pltpu.VMEM((rows, 128), F32),
                pltpu.VMEM((8, n_q), F32),
                pltpu.VMEM((8, n_q), F32),
                pltpu.VMEM((HEAD_DIM, n_q), F32),
                pltpu.VMEM((rows, d_model), BF16),
                pltpu.VMEM((rows, n_q), BF16),
                pltpu.VMEM((rows, ffn), BF16),
                pltpu.VMEM((rows, HEAD_DIM), BF16),
                pltpu.VMEM((rows, HEAD_DIM), BF16),
                pltpu.VMEM((n_t, rows, tw), BF16),
                pltpu.VMEM((n_t, rows, tw), BF16),
                pltpu.VMEM((n_t, rows, tw), BF16),
                pltpu.VMEM((n_t, rows, tw), BF16),
                dma((2,)), dma((2,)), dma((9,)), dma((9,)), dma((16,)),
                dma((3, N_SEM)), dma((2, 3, N_SEM)), dma((2, n_t)), dma((2, n_t)), dma((2,)),
            ],
            compiler_params=pltpu.CompilerParams(collective_id=0, has_side_effects=True, vmem_limit_bytes=67043328),
        )(hidden_in, aux, attn_gain.astype(F32)[:, None, :], mlp_gain.astype(F32)[:, None, :], w_q, w_k, w_v, w_o, w_gate, w_up, w_down)
        return hid, k_c.reshape(n_layers, rows, 1, HEAD_DIM), v_c.reshape(n_layers, rows, 1, HEAD_DIM)

    return jax.shard_map(device_fn, mesh=mesh,
                         in_specs=(P(('dp', 'sp', 'tp'), None), tok_spec, tok_spec, P(), col_spec, col_spec, col_spec, row_spec, P(), col_spec, col_spec, row_spec),
                         out_specs=(P(('dp', 'sp', 'tp'), None), cache_spec, cache_spec), check_vma=False)
```

```python
import math
import jax
import jax.numpy as jnp
from jax import lax
from jax.experimental import pallas as pl
from jax.experimental.pallas import tpu as pltpu
from jax.sharding import PartitionSpec as P

HEAD_DIM = 128
ROPE_BASE = 1e4
NORM_EPS = 1e-5
SCORE_SCALE = HEAD_DIM ** -0.5
EXP_SCALE = SCORE_SCALE * math.log2(math.e)
BIG = 1e30
MESH = pl.DeviceIdType.MESH
F32 = jnp.float32
BF16 = jnp.bfloat16

PART_ROWS = (48, 48, 32)
PART_OFF = (0, 48, 96)
X, Y, Z = range(3)
AXIS_STRIDE = (1, 4, 16)
PART_AXES = (((X, Y, Z), (Y, Z, X), (X, Z, Y)), ((Z, Y, X), (X, Z, Y), (X, Y, Z)))
N_SEM = 23
OWN, NEXT, FAR, PREV = range(4)
RING = 4
LANES = 128


def rms_rows(x_val, gain_row):
    x32 = x_val.astype(F32)
    inv_rms = lax.rsqrt(jnp.mean(x32 * x32, axis=-1, keepdims=True) + NORM_EPS)
    return (x32 * inv_rms * gain_row).astype(BF16)


def stack_kernel(n_layers, rows, half_rows, hid_ref, aux_ref, ga_ref, gm_ref, wq_h, wk_h, wv_h, wo_h, wg_h, wu_h, wd_h,
                 hid_out, k_out, v_out,
                 x_buf, aux_buf, cnt_buf, wqkv, wo, wg, wu, wd, kv0, kv1, kv2, ext0, ext1, ext2, q_t, mask_add,
                 m_s, l_s, acc_s, n_s, o_s, act_s, kst, vst, snd_a, rcv_a, snd_b, rcv_b,
                 gain_s, ini_ss, ini_rs, cnt_ss, cnt_rs, w_sem, g_ss, g_rs, x_ss, x_rs, c_sem):
    sp = lax.axis_index('sp')
    tp = lax.axis_index('tp')
    kvs = (kv0, kv1, kv2)
    exts = (ext0, ext1, ext2)
    n_q = wq_h.shape[2]
    n_heads = n_q // HEAD_DIM
    d_model = hid_ref.shape[1]
    ffn = wg_h.shape[2]

    axis_at = [(sp // stride) % RING for stride in AXIS_STRIDE]

    def by_core(pair):
        return pair[0] + (pair[1] - pair[0]) * tp

    ways = [[(by_core([AXIS_STRIDE[PART_AXES[core][p][d]] for core in range(2)]),
              by_core([axis_at[PART_AXES[core][p][d]] for core in range(2)])) for d in range(3)] for p in range(3)]
    coords = [tuple(at for _, at in way) for way in ways]

    def ring_to(way, delta):
        stride, here = way
        return sp + ((here + delta) % RING - here) * stride

    def remote(src, dst, ss, rs, sp_to, tp_to):
        return pltpu.make_async_remote_copy(src_ref=src, dst_ref=dst, send_sem=ss, recv_sem=rs,
                                            device_id={'sp': sp_to, 'tp': tp_to}, device_id_type=MESH)

    n_split = 4
    gr = d_model // n_split
    dr = ffn // n_split

    def qkv_copies(layer):
        nk = wk_h.shape[2]
        return [pltpu.make_async_copy(wq_h.at[layer], wqkv.at[:, 0:n_q], w_sem.at[0]),
                pltpu.make_async_copy(wk_h.at[layer], wqkv.at[:, n_q:n_q + nk], w_sem.at[1]),
                pltpu.make_async_copy(wv_h.at[layer], wqkv.at[:, n_q + nk:n_q + 2 * nk], w_sem.at[2])]

    def wo_copies(layer):
        return [pltpu.make_async_copy(wo_h.at[layer], wo, w_sem.at[3])]

    def gu_copies(layer):
        out = []
        for c in range(n_split):
            r = pl.ds(c * gr, gr)
            out.append(pltpu.make_async_copy(wg_h.at[layer, r], wg.at[r], w_sem.at[4 + c]))
            out.append(pltpu.make_async_copy(wu_h.at[layer, r], wu.at[r], w_sem.at[4 + n_split + c]))
        return out

    def down_copies(layer):
        out = []
        for c in range(n_split):
            r = pl.ds(c * dr, dr)
            out.append(pltpu.make_async_copy(wd_h.at[layer, r], wd.at[r], w_sem.at[4 + 2 * n_split + c]))
        return out

    def start_all(copies):
        for c in copies:
            c.start()

    def wait_all(copies):
        for c in copies:
            c.wait()

    start_all(qkv_copies(0))
    start_all(wo_copies(0))
    start_all(gu_copies(0))
    start_all(down_copies(0))

    gain_s[0] = ga_ref[...].astype(F32)
    gain_s[1] = gm_ref[...].astype(F32)

    barrier = pltpu.get_barrier_semaphore()
    for way in zip(AXIS_STRIDE, axis_at):
        for delta in (NEXT, FAR, PREV):
            pl.semaphore_signal(barrier, inc=1, device_id={'sp': ring_to(way, delta), 'tp': tp}, device_id_type=MESH)
    pl.semaphore_signal(barrier, inc=1, device_id={'sp': sp, 'tp': 1 - tp}, device_id_type=MESH)
    pl.semaphore_wait(barrier, 10)

    mine = pl.ds(pl.multiple_of(tp * half_rows, half_rows), half_rows)
    theirs = pl.ds(pl.multiple_of((1 - tp) * half_rows, half_rows), half_rows)
    swaps = [remote(hid_ref, x_buf.at[mine], ini_ss.at[0], ini_rs.at[0], sp, 1 - tp),
             remote(aux_ref, aux_buf.at[:, mine], ini_ss.at[1], ini_rs.at[1], sp, 1 - tp)]
    start_all(swaps)
    x_buf[mine, :] = hid_ref[...]
    for a in range(3):
        aux_buf[a, mine, :] = aux_ref[a]
    for s in swaps:
        s.wait_send()
    remote(hid_ref, x_buf.at[theirs], ini_ss.at[0], ini_rs.at[0], sp, 1 - tp).wait_recv()
    remote(aux_ref, aux_buf.at[:, theirs], ini_ss.at[1], ini_rs.at[1], sp, 1 - tp).wait_recv()

    seg_col = aux_buf[2]
    lane_f = lax.broadcasted_iota(jnp.int32, (rows, LANES), 1).astype(F32)
    below = jnp.sum(jnp.where(seg_col < lane_f, 1.0, 0.0), axis=0, keepdims=True)
    upto = jnp.sum(jnp.where(seg_col < lane_f + 1.0, 1.0, 0.0), axis=0, keepdims=True)
    mx, my, mz = axis_at
    cnt_buf[mz, my, mx] = jnp.concatenate([jnp.broadcast_to(below, (8, 128)), jnp.broadcast_to(upto, (8, 128))], axis=0)

    def count_block(phase, cz, cy, cx):
        return (cnt_buf.at[cz, cy, cx], cnt_buf.at[cz, cy], cnt_buf.at[cz])[phase]

    def count_send(phase):
        for delta in (NEXT, FAR, PREV):
            b = count_block(phase, mz, my, mx)
            i = phase * 3 + delta - 1
            remote(b, b, cnt_ss.at[i], cnt_rs.at[i], ring_to((AXIS_STRIDE[phase], axis_at[phase]), delta), tp).start()

    def count_phase(phase):
        for delta in (NEXT, FAR, PREV):
            i = phase * 3 + delta - 1
            frm = [mz, my, mx]
            frm[2 - phase] = (frm[2 - phase] - delta) % 4
            b = count_block(phase, *frm)
            c = remote(b, b, cnt_ss.at[i], cnt_rs.at[i], ring_to((AXIS_STRIDE[phase], axis_at[phase]), delta), tp)
            c.wait_send()
            c.wait_recv()
        if phase < 2:
            count_send(phase + 1)

    count_send(0)

    def fill_exts():
        total = jnp.sum(cnt_buf[...].reshape(64, 16, 128), axis=0)
        seg_lo = total[0:1, :]
        seg_hi = total[8:9, :]
        for p in range(3):
            (s1, _), (s2, _), (s3, _) = ways[p]
            pr = PART_ROWS[p]
            row_i = lax.broadcasted_iota(jnp.int32, (pr, LANES), 0)
            lane_i = lax.broadcasted_iota(jnp.int32, (pr, LANES), 1)
            row_f = row_i.astype(F32)

            def fill(b, carry, p=p, s1=s1, s2=s2, s3=s3, pr=pr, row_i=row_i, lane_i=lane_i, row_f=row_f):
                for c1 in range(4):
                    c3 = b // 4
                    c2 = b % 4
                    blk = c3 * s3 + c2 * s2 + c1 * s1
                    idx = (row_i + (blk * rows + PART_OFF[p])).astype(F32)
                    one_hot = jnp.where(idx >= seg_lo, 1.0, 0.0) * jnp.where(idx < seg_hi, 1.0, 0.0)
                    late = jnp.where(row_i * 0 + blk >= sp, 1.0, 0.0)
                    val = jnp.where(lane_i < 4, one_hot, jnp.where(lane_i == 4, late, 0.0))
                    exts[p][c3, c2, c1] = val.astype(BF16)
                return carry
            lax.fori_loop(0, 16, fill, 0)

    seg_row = jnp.transpose(seg_col)
    row_i = lax.broadcasted_iota(jnp.int32, (rows, LANES), 0)
    col_i = lax.broadcasted_iota(jnp.int32, (rows, LANES), 1)
    q_side = jnp.where(row_i < 4, jnp.where(seg_row == row_i.astype(F32), 0.0, -BIG), jnp.where(row_i == 4, -BIG, 0.0)).astype(BF16)
    for h in range(n_heads):
        q_t[128:256, h * LANES:(h + 1) * LANES] = q_side
    mask_add[...] = jnp.where(row_i <= col_i, jnp.where(seg_col == seg_row, 0.0, -BIG), -BIG)

    def soft_step(keys, vals, cols, add, first):
        n_c = cols.stop - cols.start
        q_rows = slice(0, keys.shape[1])
        s = jnp.dot(keys, q_t[q_rows, cols], preferred_element_type=F32)
        if add is not None:
            s = s + add
        top = jnp.max(s, axis=0, keepdims=True)
        if first:
            m_new = top
        else:
            m_old = m_s[0:1, cols]
            m_new = jnp.maximum(m_old, top)
        e = jnp.exp2((s - m_new) * EXP_SCALE)
        e_sum = jnp.sum(e, axis=0, keepdims=True)
        pv = lax.dot_general(vals, e.astype(BF16), (((0,), (0,)), ((), ())), preferred_element_type=F32)
        if first:
            l_new = e_sum
            acc_s[:, cols] = pv
        else:
            alpha = jnp.exp2((m_old - m_new) * EXP_SCALE)
            l_new = l_s[0:1, cols] * alpha + e_sum
            acc_s[:, cols] = acc_s[:, cols] * alpha + pv
        m_s[:, cols] = jnp.broadcast_to(m_new, (8, n_c))
        l_s[:, cols] = jnp.broadcast_to(l_new, (8, n_c))

    base2 = 3
    base3 = base2 + RING
    first_two = pl.ds(0, 2)
    last_two = pl.ds(2, 2)
    col_tiles = [slice(c, c + 256) for c in range(0, n_q, 256)]

    def row_step(par, coords, o3, o2):
        kv_rows, ext_rows = [], []
        for p in range(3):
            m1, m2, m3 = coords[p]
            c3 = (m3 + o3) % RING
            c2 = (m2 + o2) % RING
            n_k = 4 * PART_ROWS[p]
            kv_rows.append(kvs[p][par, c3, c2].reshape(n_k, 256))
            ext_rows.append(exts[p][c3, c2].reshape(n_k, 128))
        kv = jnp.concatenate(kv_rows, axis=0)
        keys = jnp.concatenate([kv[:, 0:128], jnp.concatenate(ext_rows, axis=0)], axis=1)
        vals = kv[:, 128:256]
        m_old = [m_s[0:1, cols] for cols in col_tiles]
        l_old = [l_s[0:1, cols] for cols in col_tiles]
        half = keys.shape[0] // 2
        parts = (slice(0, half), slice(half, 2 * half))
        ss = [[jnp.dot(keys[r], q_t[:, cols], preferred_element_type=F32) for r in parts] for cols in col_tiles]
        m_new = [jnp.maximum(a, jnp.max(jnp.maximum(b[0], b[1]), axis=0, keepdims=True)) for a, b in zip(m_old, ss)]
        es = [[jnp.exp2((b - a) * EXP_SCALE) for b in bs] for a, bs in zip(m_new, ss)]
        al = [jnp.exp2((a - b) * EXP_SCALE) for a, b in zip(m_old, m_new)]
        vt = jnp.transpose(vals)
        pvs = [jnp.dot(vt[:, 0:half], e[0].astype(BF16), preferred_element_type=F32) + jnp.dot(vt[:, half:], e[1].astype(BF16), preferred_element_type=F32) for e in es]
        for i, cols in enumerate(col_tiles):
            l_new = l_old[i] * al[i] + jnp.sum(es[i][0] + es[i][1], axis=0, keepdims=True)
            acc_s[:, cols] = acc_s[:, cols] * al[i] + pvs[i]
            m_s[:, cols] = jnp.broadcast_to(m_new[i], (8, 256))
            l_s[:, cols] = jnp.broadcast_to(l_new, (8, 256))

    def layer_step(layer, carry):
        par = layer % 2
        has_next = layer + 1 < n_layers

        def send(p, i, ref, dim, delta):
            remote(ref, ref, g_ss.at[p, i], g_rs.at[par, p, i], ring_to(ways[p][dim], delta), tp).start()

        def got(p, i, ref):
            remote(ref, ref, g_ss.at[p, i], g_rs.at[par, p, i], sp, 1 - tp).wait_recv()

        def sent(p, i, ref):
            remote(ref, ref, g_ss.at[p, i], g_rs.at[par, p, i], sp, 1 - tp).wait_send()

        def first_layer(step, *a):
            @pl.when(layer == 0)
            def _():
                step(*a)

        n_s[...] = rms_rows(x_buf[...], gain_s[0, pl.ds(layer, 1), :])
        wait_all(qkv_copies(layer))
        cos_t = aux_buf[0]
        sin_t = aux_buf[1]

        def rope(v):
            return (v * cos_t + pltpu.roll(v, HEAD_DIM // 2, 1) * sin_t).astype(BF16)

        kv_lin = jnp.dot(n_s[...], wqkv[:, n_q:], preferred_element_type=F32)
        k_rot = rope(kv_lin[:, 0:128])
        v_val = kv_lin[:, 128:256].astype(BF16)
        kst[...] = k_rot
        vst[...] = v_val
        kv_val = jnp.concatenate([k_rot, v_val], axis=1)
        for p in range(3):
            m1, m2, m3 = coords[p]
            kvs[p][par, m3, m2, m1] = kv_val[PART_OFF[p]:PART_OFF[p] + PART_ROWS[p], :]
        cache = [pltpu.make_async_copy(kst, k_out.at[layer], c_sem.at[0]),
                 pltpu.make_async_copy(vst, v_out.at[layer], c_sem.at[1])]
        start_all(cache)
        for p in range(3):
            m1, m2, m3 = coords[p]
            for delta in (FAR, NEXT, PREV):
                send(p, delta - 1, kvs[p].at[par, m3, m2, m1], 0, delta)
        q_lin = jnp.dot(n_s[...], wqkv[:, 0:n_q], preferred_element_type=F32)
        for h in range(n_heads):
            q_h = rope(q_lin[:, h * LANES:(h + 1) * LANES])
            q_t[0:128, h * LANES:(h + 1) * LANES] = jnp.transpose(q_h)

        @pl.when(has_next)
        def _():
            start_all(qkv_copies(layer + 1))

        first_layer(count_phase, 0)

        mask2 = jnp.concatenate([mask_add[...], mask_add[...]], axis=1)
        for cols in col_tiles:
            soft_step(kst[...], vst[...], cols, mask2, True)

        first_layer(count_phase, 1)
        def ring_sends(p, base, dim, ref):
            send(p, base, ref, dim, NEXT)
            send(p, base + 1, ref, dim, PREV)

        def row_sems(off):
            return base3 + RING * off

        for p in range(3):
            m1, m2, m3 = coords[p]
            for delta in (NEXT, PREV, FAR):
                got(p, delta - 1, kvs[p].at[par, m3, m2, (m1 - delta) % RING])
            row = kvs[p].at[par, m3, m2]
            ring_sends(p, base2, 1, row)
            ring_sends(p, row_sems(OWN), 2, row)
        first_layer(count_phase, 2)
        first_layer(fill_exts)
        row_step(par, coords, OWN, OWN)

        def ring_pass(p, base, dim, prev, nxt):
            got(p, base, prev)
            send(p, base + 2, prev.at[first_two], dim, NEXT)
            got(p, base + 1, nxt)
            send(p, base + 3, nxt.at[last_two], dim, PREV)

        def ring_far(p, base, far):
            got(p, base + 2, far.at[first_two])
            got(p, base + 3, far.at[last_two])

        def row_at(p, o3, o2):
            m1, m2, m3 = coords[p]
            return kvs[p].at[par, (m3 + o3) % RING, (m2 + o2) % RING]

        def pass_on3(off):
            for p in range(3):
                ring_pass(p, row_sems(off), 2, row_at(p, PREV, off), row_at(p, NEXT, off))

        def far3(off):
            for p in range(3):
                ring_far(p, row_sems(off), row_at(p, FAR, off))

        for p in range(3):
            ring_pass(p, base2, 1, row_at(p, OWN, PREV), row_at(p, OWN, NEXT))
            for off in (PREV, NEXT):
                ring_sends(p, row_sems(off), 2, row_at(p, OWN, off))
        row_step(par, coords, OWN, PREV)
        pass_on3(OWN)
        row_step(par, coords, OWN, NEXT)
        for p in range(3):
            ring_far(p, base2, row_at(p, OWN, FAR))
            ring_sends(p, row_sems(FAR), 2, row_at(p, OWN, FAR))
        row_step(par, coords, PREV, OWN)
        row_step(par, coords, NEXT, OWN)
        pass_on3(PREV)
        row_step(par, coords, OWN, FAR)
        row_step(par, coords, PREV, PREV)
        pass_on3(NEXT)
        row_step(par, coords, NEXT, PREV)
        far3(OWN)
        row_step(par, coords, FAR, OWN)
        row_step(par, coords, PREV, NEXT)
        pass_on3(FAR)
        row_step(par, coords, NEXT, NEXT)
        row_step(par, coords, PREV, FAR)
        row_step(par, coords, NEXT, FAR)
        far3(PREV)
        row_step(par, coords, FAR, PREV)
        far3(NEXT)
        row_step(par, coords, FAR, NEXT)
        far3(FAR)
        row_step(par, coords, FAR, FAR)

        for h in range(n_heads):
            cols = slice(h * LANES, (h + 1) * LANES)
            o_t = acc_s[:, cols] * (1.0 / l_s[0:1, cols])
            o_s[:, cols] = jnp.transpose(o_t.astype(BF16))
        wait_all(wo_copies(layer))
        n_t = snd_a.shape[0]
        tw = snd_a.shape[2]
        swap_a = [remote(snd_a.at[t], rcv_a.at[t], x_ss.at[0, t], x_rs.at[0, t], sp, 1 - tp) for t in range(n_t)]
        swap_b = [remote(snd_b.at[t], rcv_b.at[t], x_ss.at[1, t], x_rs.at[1, t], sp, 1 - tp) for t in range(n_t)]
        for t in range(n_t):
            part = jnp.dot(o_s[...], wo[:, t * tw:(t + 1) * tw], preferred_element_type=F32)
            snd_a[t] = part.astype(BF16)
            swap_a[t].start()

        for p in range(3):
            m1, m2, m3 = coords[p]
            row = kvs[p].at[par, m3, m2]
            for i in range(base2):
                sent(p, i, row.at[m1])
            for base in (base2, *map(row_sems, range(RING))):
                for i in range(2):
                    sent(p, base + i, row)
                    sent(p, base + 2 + i, row.at[first_two])

        @pl.when(has_next)
        def _():
            start_all(wo_copies(layer + 1))

        for t in range(n_t):
            swap_a[t].wait()
            cols = slice(t * tw, (t + 1) * tw)
            res = (snd_a[t].astype(F32) + rcv_a[t].astype(F32)).astype(BF16)
            x_buf[:, cols] = (x_buf[:, cols].astype(F32) + res.astype(F32)).astype(BF16)

        n_s[...] = rms_rows(x_buf[...], gain_s[1, pl.ds(layer, 1), :])
        wait_all(gu_copies(layer))

        def gate_up(cols):
            gate = jnp.dot(n_s[...], wg[:, cols], preferred_element_type=F32)
            up = jnp.dot(n_s[...], wu[:, cols], preferred_element_type=F32)
            act_s[:, cols] = (gate * jax.nn.sigmoid(gate) * up).astype(BF16)

        gt = 1024

        def gate_up_tile(t, c):
            gate_up(pl.ds(pl.multiple_of(t * gt, gt), gt))
            return c
        n_full = ffn // gt
        lax.fori_loop(0, n_full, gate_up_tile, 0)
        if ffn % gt:
            gate_up(slice(n_full * gt, ffn))

        @pl.when(has_next)
        def _():
            start_all(gu_copies(layer + 1))

        wait_all(down_copies(layer))
        for t in range(n_t):
            part = jnp.dot(act_s[...], wd[:, t * tw:(t + 1) * tw], preferred_element_type=F32)
            snd_b[t] = part.astype(BF16)
            swap_b[t].start()

        @pl.when(has_next)
        def _():
            start_all(down_copies(layer + 1))

        wait_all(cache)
        for t in range(n_t):
            swap_b[t].wait()
            cols = slice(t * tw, (t + 1) * tw)
            res = (snd_b[t].astype(F32) + rcv_b[t].astype(F32)).astype(BF16)
            x_buf[:, cols] = (x_buf[:, cols].astype(F32) + res.astype(F32)).astype(BF16)
        return carry

    lax.fori_loop(0, n_layers, layer_step, 0)
    hid_out[...] = x_buf[mine, :]


def solution(mesh):
    tok_spec = P(('dp', 'sp', 'tp'))
    col_spec = P(None, None, 'tp')
    row_spec = P(None, 'tp', None)
    cache_spec = P(None, ('dp', 'sp'), 'tp', None)

    def device_fn(hidden_in, segment_ids, positions, attn_gain, w_q, w_k, w_v, w_o, mlp_gain, w_gate, w_up, w_down):
        half_rows, d_model = hidden_in.shape
        rows = 2 * half_rows
        n_layers, _, n_q = w_q.shape
        ffn = w_gate.shape[2]
        half_dim = HEAD_DIM // 2
        inv_freq = ROPE_BASE ** (-jnp.arange(half_dim, dtype=F32) / half_dim)
        angles = positions.astype(F32)[:, None] * inv_freq
        cos_val = jnp.cos(angles)
        sin_val = jnp.sin(angles)
        aux = jnp.stack([jnp.concatenate([cos_val, cos_val], axis=1), jnp.concatenate([-sin_val, sin_val], axis=1),
                         jnp.broadcast_to(segment_ids.astype(F32)[:, None], (half_rows, HEAD_DIM))])
        vm = pl.BlockSpec(memory_space=pltpu.VMEM)
        anyspec = pl.BlockSpec(memory_space=pl.ANY)
        n_t, tw = 3, d_model // 3
        dma = pltpu.SemaphoreType.DMA
        body = lambda *refs: stack_kernel(n_layers, rows, half_rows, *refs)
        hid, k_c, v_c = pl.pallas_call(
            body,
            out_shape=(jax.ShapeDtypeStruct((half_rows, d_model), BF16),
                       jax.ShapeDtypeStruct((n_layers, rows, HEAD_DIM), BF16),
                       jax.ShapeDtypeStruct((n_layers, rows, HEAD_DIM), BF16)),
            in_specs=[vm, vm, vm, vm] + [anyspec] * 7,
            out_specs=(vm, anyspec, anyspec),
            scratch_shapes=[
                pltpu.VMEM((rows, d_model), BF16),
                pltpu.VMEM((3, rows, 128), F32),
                pltpu.VMEM((4, 4, 4, 16, 128), F32),
                pltpu.VMEM((d_model, n_q + 2 * HEAD_DIM), BF16),
                pltpu.VMEM((n_q, d_model), BF16),
                pltpu.VMEM((d_model, ffn), BF16),
                pltpu.VMEM((d_model, ffn), BF16),
                pltpu.VMEM((ffn, d_model), BF16),
                *[pltpu.VMEM((2, RING, RING, RING, r, 2 * LANES), BF16) for r in PART_ROWS],
                *[pltpu.VMEM((RING, RING, RING, r, LANES), BF16) for r in PART_ROWS],
                pltpu.VMEM((256, n_q), BF16),
                pltpu.VMEM((rows, LANES), F32),
                pltpu.VMEM((8, n_q), F32),
                pltpu.VMEM((8, n_q), F32),
                pltpu.VMEM((HEAD_DIM, n_q), F32),
                pltpu.VMEM((rows, d_model), BF16),
                pltpu.VMEM((rows, n_q), BF16),
                pltpu.VMEM((rows, ffn), BF16),
                pltpu.VMEM((rows, HEAD_DIM), BF16),
                pltpu.VMEM((rows, HEAD_DIM), BF16),
                pltpu.VMEM((n_t, rows, tw), BF16),
                pltpu.VMEM((n_t, rows, tw), BF16),
                pltpu.VMEM((n_t, rows, tw), BF16),
                pltpu.VMEM((n_t, rows, tw), BF16),
                pltpu.VMEM((2, n_layers, d_model), F32),
                dma((2,)), dma((2,)), dma((9,)), dma((9,)), dma((16,)),
                dma((3, N_SEM)), dma((2, 3, N_SEM)), dma((2, n_t)), dma((2, n_t)), dma((2,)),
            ],
            compiler_params=pltpu.CompilerParams(collective_id=0, has_side_effects=True, vmem_limit_bytes=67043328),
        )(hidden_in, aux, attn_gain, mlp_gain, w_q, w_k, w_v, w_o, w_gate, w_up, w_down)
        return hid, k_c.reshape(n_layers, rows, 1, HEAD_DIM), v_c.reshape(n_layers, rows, 1, HEAD_DIM)

    return jax.shard_map(device_fn, mesh=mesh,
                         in_specs=(P(('dp', 'sp', 'tp'), None), tok_spec, tok_spec, P(), col_spec, col_spec, col_spec, row_spec, P(), col_spec, col_spec, row_spec),
                         out_specs=(P(('dp', 'sp', 'tp'), None), cache_spec, cache_spec), check_vma=False)
```

```python
import math
import jax
import jax.numpy as jnp
from jax import lax
from jax.experimental import pallas as pl
from jax.experimental.pallas import tpu as pltpu
from jax.sharding import PartitionSpec as P

HEAD_DIM = 128
ROPE_BASE = 1e4
NORM_EPS = 1e-5
SCORE_SCALE = HEAD_DIM ** -0.5
EXP_SCALE = SCORE_SCALE * math.log2(math.e)
BIG = 1e30
MESH = pl.DeviceIdType.MESH
F32 = jnp.float32
BF16 = jnp.bfloat16

PART_ROWS = (48, 48, 32)
PART_OFF = (0, 48, 96)
X, Y, Z = range(3)
AXIS_STRIDE = (1, 4, 16)
PART_AXES = (((X, Y, Z), (Y, Z, X), (Z, X, Y)), ((Y, Z, X), (Z, X, Y), (X, Y, Z)))
N_SEM = 23
OWN, NEXT, FAR, PREV = range(4)
RING = 4
LANES = 128


def rms_rows(x_val, gain_row):
    x32 = x_val.astype(F32)
    inv_rms = lax.rsqrt(jnp.mean(x32 * x32, axis=-1, keepdims=True) + NORM_EPS)
    return (x32 * inv_rms * gain_row).astype(BF16)


def stack_kernel(n_layers, rows, half_rows, hid_ref, aux_ref, ga_ref, gm_ref, wq_h, wk_h, wv_h, wo_h, wg_h, wu_h, wd_h,
                 hid_out, k_out, v_out,
                 x_buf, aux_buf, cnt_buf, wqkv, wo, wg, wu, wd, kv0, kv1, kv2, ext0, ext1, ext2, q_t, mask_add,
                 m_s, l_s, acc_s, n_s, o_s, act_s, kst, vst, snd_a, rcv_a, snd_b, rcv_b,
                 gain_s, ini_ss, ini_rs, cnt_ss, cnt_rs, w_sem, g_ss, g_rs, x_ss, x_rs, c_sem):
    sp = lax.axis_index('sp')
    tp = lax.axis_index('tp')
    kvs = (kv0, kv1, kv2)
    exts = (ext0, ext1, ext2)
    n_q = wq_h.shape[2]
    n_heads = n_q // HEAD_DIM
    d_model = hid_ref.shape[1]
    ffn = wg_h.shape[2]

    axis_at = [(sp // stride) % RING for stride in AXIS_STRIDE]

    def by_core(pair):
        return pair[0] + (pair[1] - pair[0]) * tp

    ways = [[(by_core([AXIS_STRIDE[PART_AXES[core][p][d]] for core in range(2)]),
              by_core([axis_at[PART_AXES[core][p][d]] for core in range(2)])) for d in range(3)] for p in range(3)]
    coords = [tuple(at for _, at in way) for way in ways]

    def ring_to(way, delta):
        stride, here = way
        return sp + ((here + delta) % RING - here) * stride

    def remote(src, dst, ss, rs, sp_to, tp_to):
        return pltpu.make_async_remote_copy(src_ref=src, dst_ref=dst, send_sem=ss, recv_sem=rs,
                                            device_id={'sp': sp_to, 'tp': tp_to}, device_id_type=MESH)

    n_split = 4
    gr = d_model // n_split
    dr = ffn // n_split

    def qkv_copies(layer):
        nk = wk_h.shape[2]
        return [pltpu.make_async_copy(wq_h.at[layer], wqkv.at[:, 0:n_q], w_sem.at[0]),
                pltpu.make_async_copy(wk_h.at[layer], wqkv.at[:, n_q:n_q + nk], w_sem.at[1]),
                pltpu.make_async_copy(wv_h.at[layer], wqkv.at[:, n_q + nk:n_q + 2 * nk], w_sem.at[2])]

    def wo_copies(layer):
        return [pltpu.make_async_copy(wo_h.at[layer], wo, w_sem.at[3])]

    def gu_copies(layer):
        out = []
        for c in range(n_split):
            r = pl.ds(c * gr, gr)
            out.append(pltpu.make_async_copy(wg_h.at[layer, r], wg.at[r], w_sem.at[4 + c]))
            out.append(pltpu.make_async_copy(wu_h.at[layer, r], wu.at[r], w_sem.at[4 + n_split + c]))
        return out

    def down_copies(layer):
        out = []
        for c in range(n_split):
            r = pl.ds(c * dr, dr)
            out.append(pltpu.make_async_copy(wd_h.at[layer, r], wd.at[r], w_sem.at[4 + 2 * n_split + c]))
        return out

    def start_all(copies):
        for c in copies:
            c.start()

    def wait_all(copies):
        for c in copies:
            c.wait()

    start_all(qkv_copies(0))
    start_all(wo_copies(0))
    start_all(gu_copies(0))
    start_all(down_copies(0))

    gain_s[0] = ga_ref[...].astype(F32)
    gain_s[1] = gm_ref[...].astype(F32)

    barrier = pltpu.get_barrier_semaphore()
    for way in zip(AXIS_STRIDE, axis_at):
        for delta in (NEXT, FAR, PREV):
            pl.semaphore_signal(barrier, inc=1, device_id={'sp': ring_to(way, delta), 'tp': tp}, device_id_type=MESH)
    pl.semaphore_signal(barrier, inc=1, device_id={'sp': sp, 'tp': 1 - tp}, device_id_type=MESH)
    pl.semaphore_wait(barrier, 10)

    mine = pl.ds(pl.multiple_of(tp * half_rows, half_rows), half_rows)
    theirs = pl.ds(pl.multiple_of((1 - tp) * half_rows, half_rows), half_rows)
    swaps = [remote(hid_ref, x_buf.at[mine], ini_ss.at[0], ini_rs.at[0], sp, 1 - tp),
             remote(aux_ref, aux_buf.at[:, mine], ini_ss.at[1], ini_rs.at[1], sp, 1 - tp)]
    start_all(swaps)
    x_buf[mine, :] = hid_ref[...]
    for a in range(3):
        aux_buf[a, mine, :] = aux_ref[a]
    for s in swaps:
        s.wait_send()
    remote(hid_ref, x_buf.at[theirs], ini_ss.at[0], ini_rs.at[0], sp, 1 - tp).wait_recv()
    remote(aux_ref, aux_buf.at[:, theirs], ini_ss.at[1], ini_rs.at[1], sp, 1 - tp).wait_recv()

    seg_col = aux_buf[2]
    lane_f = lax.broadcasted_iota(jnp.int32, (rows, LANES), 1).astype(F32)
    below = jnp.sum(jnp.where(seg_col < lane_f, 1.0, 0.0), axis=0, keepdims=True)
    upto = jnp.sum(jnp.where(seg_col < lane_f + 1.0, 1.0, 0.0), axis=0, keepdims=True)
    mx, my, mz = axis_at
    cnt_buf[mz, my, mx] = jnp.concatenate([jnp.broadcast_to(below, (8, 128)), jnp.broadcast_to(upto, (8, 128))], axis=0)

    def count_block(phase, cz, cy, cx):
        return (cnt_buf.at[cz, cy, cx], cnt_buf.at[cz, cy], cnt_buf.at[cz])[phase]

    def count_send(phase):
        for delta in (NEXT, FAR, PREV):
            b = count_block(phase, mz, my, mx)
            i = phase * 3 + delta - 1
            remote(b, b, cnt_ss.at[i], cnt_rs.at[i], ring_to((AXIS_STRIDE[phase], axis_at[phase]), delta), tp).start()

    def count_phase(phase):
        for delta in (NEXT, FAR, PREV):
            i = phase * 3 + delta - 1
            frm = [mz, my, mx]
            frm[2 - phase] = (frm[2 - phase] - delta) % 4
            b = count_block(phase, *frm)
            c = remote(b, b, cnt_ss.at[i], cnt_rs.at[i], ring_to((AXIS_STRIDE[phase], axis_at[phase]), delta), tp)
            c.wait_send()
            c.wait_recv()
        if phase < 2:
            count_send(phase + 1)

    count_send(0)

    def fill_exts():
        total = jnp.sum(cnt_buf[...].reshape(64, 16, 128), axis=0)
        seg_lo = total[0:1, :]
        seg_hi = total[8:9, :]
        for p in range(3):
            (s1, _), (s2, _), (s3, _) = ways[p]
            pr = PART_ROWS[p]
            row_i = lax.broadcasted_iota(jnp.int32, (pr, LANES), 0)
            lane_i = lax.broadcasted_iota(jnp.int32, (pr, LANES), 1)
            row_f = row_i.astype(F32)

            def fill(b, carry, p=p, s1=s1, s2=s2, s3=s3, pr=pr, row_i=row_i, lane_i=lane_i, row_f=row_f):
                for c1 in range(4):
                    c3 = b // 4
                    c2 = b % 4
                    blk = c3 * s3 + c2 * s2 + c1 * s1
                    idx = (row_i + (blk * rows + PART_OFF[p])).astype(F32)
                    one_hot = jnp.where(idx >= seg_lo, 1.0, 0.0) * jnp.where(idx < seg_hi, 1.0, 0.0)
                    late = jnp.where(row_i * 0 + blk >= sp, 1.0, 0.0)
                    val = jnp.where(lane_i < 4, one_hot, jnp.where(lane_i == 4, late, 0.0))
                    exts[p][c3, c2, c1] = val.astype(BF16)
                return carry
            lax.fori_loop(0, 16, fill, 0)

    seg_row = jnp.transpose(seg_col)
    row_i = lax.broadcasted_iota(jnp.int32, (rows, LANES), 0)
    col_i = lax.broadcasted_iota(jnp.int32, (rows, LANES), 1)
    q_side = jnp.where(row_i < 4, jnp.where(seg_row == row_i.astype(F32), 0.0, -BIG), jnp.where(row_i == 4, -BIG, 0.0)).astype(BF16)
    for h in range(n_heads):
        q_t[128:256, h * LANES:(h + 1) * LANES] = q_side
    mask_add[...] = jnp.where(row_i <= col_i, jnp.where(seg_col == seg_row, 0.0, -BIG), -BIG)

    def soft_step(keys, vals, cols, add, first):
        n_c = cols.stop - cols.start
        q_rows = slice(0, keys.shape[1])
        s = jnp.dot(keys, q_t[q_rows, cols], preferred_element_type=F32)
        if add is not None:
            s = s + add
        top = jnp.max(s, axis=0, keepdims=True)
        if first:
            m_new = top
        else:
            m_old = m_s[0:1, cols]
            m_new = jnp.maximum(m_old, top)
        e = jnp.exp2((s - m_new) * EXP_SCALE)
        e_sum = jnp.sum(e, axis=0, keepdims=True)
        pv = lax.dot_general(vals, e.astype(BF16), (((0,), (0,)), ((), ())), preferred_element_type=F32)
        if first:
            l_new = e_sum
            acc_s[:, cols] = pv
        else:
            alpha = jnp.exp2((m_old - m_new) * EXP_SCALE)
            l_new = l_s[0:1, cols] * alpha + e_sum
            acc_s[:, cols] = acc_s[:, cols] * alpha + pv
        m_s[:, cols] = jnp.broadcast_to(m_new, (8, n_c))
        l_s[:, cols] = jnp.broadcast_to(l_new, (8, n_c))

    base2 = 3
    base3 = base2 + RING
    first_two = pl.ds(0, 2)
    last_two = pl.ds(2, 2)
    col_tiles = [slice(c, c + 256) for c in range(0, n_q, 256)]

    def row_step(par, coords, *offs):
        kv_rows, ext_rows = [], []
        for o3, o2 in offs:
            for p in range(3):
                m1, m2, m3 = coords[p]
                c3 = (m3 + o3) % RING
                c2 = (m2 + o2) % RING
                n_k = RING * PART_ROWS[p]
                kv_rows.append(kvs[p][par, c3, c2].reshape(n_k, 256))
                ext_rows.append(exts[p][c3, c2].reshape(n_k, LANES))
        kv = jnp.concatenate(kv_rows, axis=0)
        keys = jnp.concatenate([kv[:, 0:128], jnp.concatenate(ext_rows, axis=0)], axis=1)
        vals = kv[:, 128:256]
        m_old = [m_s[0:1, cols] for cols in col_tiles]
        l_old = [l_s[0:1, cols] for cols in col_tiles]
        half = keys.shape[0] // 2
        parts = (slice(0, half), slice(half, 2 * half))
        ss = [[jnp.dot(keys[r], q_t[:, cols], preferred_element_type=F32) for r in parts] for cols in col_tiles]
        m_new = [jnp.maximum(a, jnp.max(jnp.maximum(b[0], b[1]), axis=0, keepdims=True)) for a, b in zip(m_old, ss)]
        es = [[jnp.exp2((b - a) * EXP_SCALE) for b in bs] for a, bs in zip(m_new, ss)]
        al = [jnp.exp2((a - b) * EXP_SCALE) for a, b in zip(m_old, m_new)]
        vt = jnp.concatenate([jnp.transpose(vals), jnp.ones((16, 2 * half), BF16)], axis=0)
        pvs = [jnp.dot(vt[:, 0:half], e[0].astype(BF16), preferred_element_type=F32) + jnp.dot(vt[:, half:], e[1].astype(BF16), preferred_element_type=F32) for e in es]
        for i, cols in enumerate(col_tiles):
            acc_s[:, cols] = acc_s[:, cols] * al[i] + pvs[i][0:LANES]
            l_s[:, cols] = l_s[:, cols] * al[i] + pvs[i][LANES:LANES + 8]
            m_s[:, cols] = jnp.broadcast_to(m_new[i], (8, 256))

    def layer_step(layer, carry):
        par = layer % 2
        has_next = layer + 1 < n_layers

        def send(p, i, ref, dim, delta):
            remote(ref, ref, g_ss.at[p, i], g_rs.at[par, p, i], ring_to(ways[p][dim], delta), tp).start()

        def got(p, i, ref):
            remote(ref, ref, g_ss.at[p, i], g_rs.at[par, p, i], sp, 1 - tp).wait_recv()

        def sent(p, i, ref):
            remote(ref, ref, g_ss.at[p, i], g_rs.at[par, p, i], sp, 1 - tp).wait_send()

        def first_layer(step, *a):
            @pl.when(layer == 0)
            def _():
                step(*a)

        n_s[...] = rms_rows(x_buf[...], gain_s[0, pl.ds(layer, 1), :])
        wait_all(qkv_copies(layer))
        cos_t = aux_buf[0]
        sin_t = aux_buf[1]

        def rope(v):
            return (v * cos_t + pltpu.roll(v, HEAD_DIM // 2, 1) * sin_t).astype(BF16)

        kv_lin = jnp.dot(n_s[...], wqkv[:, n_q:], preferred_element_type=F32)
        k_rot = rope(kv_lin[:, 0:128])
        v_val = kv_lin[:, 128:256].astype(BF16)
        kst[...] = k_rot
        vst[...] = v_val
        kv_val = jnp.concatenate([k_rot, v_val], axis=1)
        for p in range(3):
            m1, m2, m3 = coords[p]
            kvs[p][par, m3, m2, m1] = kv_val[PART_OFF[p]:PART_OFF[p] + PART_ROWS[p], :]
        cache = [pltpu.make_async_copy(kst, k_out.at[layer], c_sem.at[0]),
                 pltpu.make_async_copy(vst, v_out.at[layer], c_sem.at[1])]
        start_all(cache)
        for p in range(3):
            m1, m2, m3 = coords[p]
            for delta in (FAR, NEXT, PREV):
                send(p, delta - 1, kvs[p].at[par, m3, m2, m1], 0, delta)
        q_lin = jnp.dot(n_s[...], wqkv[:, 0:n_q], preferred_element_type=F32)
        for h in range(n_heads):
            q_h = rope(q_lin[:, h * LANES:(h + 1) * LANES])
            q_t[0:128, h * LANES:(h + 1) * LANES] = jnp.transpose(q_h)

        @pl.when(has_next)
        def _():
            start_all(qkv_copies(layer + 1))

        first_layer(count_phase, 0)

        mask2 = jnp.concatenate([mask_add[...], mask_add[...]], axis=1)
        for cols in col_tiles:
            soft_step(kst[...], vst[...], cols, mask2, True)

        first_layer(count_phase, 1)
        def ring_sends(p, base, dim, ref):
            send(p, base, ref, dim, NEXT)
            send(p, base + 1, ref, dim, PREV)

        def row_sems(off):
            return base3 + RING * off

        for p in range(3):
            m1, m2, m3 = coords[p]
            for delta in (NEXT, PREV, FAR):
                got(p, delta - 1, kvs[p].at[par, m3, m2, (m1 - delta) % RING])
            row = kvs[p].at[par, m3, m2]
            ring_sends(p, base2, 1, row)
            ring_sends(p, row_sems(OWN), 2, row)
        first_layer(count_phase, 2)
        first_layer(fill_exts)
        row_step(par, coords, (OWN, OWN))

        def ring_pass(p, base, dim, prev, nxt):
            got(p, base, prev)
            send(p, base + 2, prev.at[first_two], dim, NEXT)
            got(p, base + 1, nxt)
            send(p, base + 3, nxt.at[last_two], dim, PREV)

        def ring_far(p, base, far):
            got(p, base + 2, far.at[first_two])
            got(p, base + 3, far.at[last_two])

        def row_at(p, o3, o2):
            m1, m2, m3 = coords[p]
            return kvs[p].at[par, (m3 + o3) % RING, (m2 + o2) % RING]

        def pass_on3(off):
            for p in range(3):
                ring_pass(p, row_sems(off), 2, row_at(p, PREV, off), row_at(p, NEXT, off))

        def far3(off):
            for p in range(3):
                ring_far(p, row_sems(off), row_at(p, FAR, off))

        for p in range(3):
            ring_pass(p, base2, 1, row_at(p, OWN, PREV), row_at(p, OWN, NEXT))
            for off in (PREV, NEXT):
                ring_sends(p, row_sems(off), 2, row_at(p, OWN, off))
        row_step(par, coords, (OWN, PREV))
        pass_on3(OWN)
        row_step(par, coords, (OWN, NEXT))
        for p in range(3):
            ring_far(p, base2, row_at(p, OWN, FAR))
            ring_sends(p, row_sems(FAR), 2, row_at(p, OWN, FAR))
        row_step(par, coords, (PREV, OWN), (NEXT, OWN))
        pass_on3(PREV)
        row_step(par, coords, (OWN, FAR))
        row_step(par, coords, (PREV, PREV))
        pass_on3(NEXT)
        row_step(par, coords, (NEXT, PREV))
        far3(OWN)
        row_step(par, coords, (FAR, OWN))
        row_step(par, coords, (PREV, NEXT))
        pass_on3(FAR)
        row_step(par, coords, (NEXT, NEXT))
        row_step(par, coords, (PREV, FAR), (NEXT, FAR))
        far3(PREV)
        far3(NEXT)
        row_step(par, coords, (FAR, PREV), (FAR, NEXT))
        far3(FAR)
        row_step(par, coords, (FAR, FAR))

        for h in range(n_heads):
            cols = slice(h * LANES, (h + 1) * LANES)
            o_t = acc_s[:, cols] * (1.0 / l_s[0:1, cols])
            o_s[:, cols] = jnp.transpose(o_t.astype(BF16))
        wait_all(wo_copies(layer))
        n_t = snd_a.shape[0]
        tw = snd_a.shape[2]
        swap_a = [remote(snd_a.at[t], rcv_a.at[t], x_ss.at[0, t], x_rs.at[0, t], sp, 1 - tp) for t in range(n_t)]
        swap_b = [remote(snd_b.at[t], rcv_b.at[t], x_ss.at[1, t], x_rs.at[1, t], sp, 1 - tp) for t in range(n_t)]
        for t in range(n_t):
            part = jnp.dot(o_s[...], wo[:, t * tw:(t + 1) * tw], preferred_element_type=F32)
            snd_a[t] = part.astype(BF16)
            swap_a[t].start()

        for p in range(3):
            m1, m2, m3 = coords[p]
            row = kvs[p].at[par, m3, m2]
            for i in range(base2):
                sent(p, i, row.at[m1])
            for base in (base2, *map(row_sems, range(RING))):
                for i in range(2):
                    sent(p, base + i, row)
                    sent(p, base + 2 + i, row.at[first_two])

        @pl.when(has_next)
        def _():
            start_all(wo_copies(layer + 1))

        for t in range(n_t):
            swap_a[t].wait()
            cols = slice(t * tw, (t + 1) * tw)
            res = (snd_a[t].astype(F32) + rcv_a[t].astype(F32)).astype(BF16)
            x_buf[:, cols] = (x_buf[:, cols].astype(F32) + res.astype(F32)).astype(BF16)

        n_s[...] = rms_rows(x_buf[...], gain_s[1, pl.ds(layer, 1), :])
        wait_all(gu_copies(layer))

        def gate_up(cols):
            gate = jnp.dot(n_s[...], wg[:, cols], preferred_element_type=F32)
            up = jnp.dot(n_s[...], wu[:, cols], preferred_element_type=F32)
            act_s[:, cols] = (gate * jax.nn.sigmoid(gate) * up).astype(BF16)

        gt = 1024

        def gate_up_tile(t, c):
            gate_up(pl.ds(pl.multiple_of(t * gt, gt), gt))
            return c
        n_full = ffn // gt
        lax.fori_loop(0, n_full, gate_up_tile, 0)
        if ffn % gt:
            gate_up(slice(n_full * gt, ffn))

        @pl.when(has_next)
        def _():
            start_all(gu_copies(layer + 1))

        wait_all(down_copies(layer))
        for t in range(n_t):
            part = jnp.dot(act_s[...], wd[:, t * tw:(t + 1) * tw], preferred_element_type=F32)
            snd_b[t] = part.astype(BF16)
            swap_b[t].start()

        @pl.when(has_next)
        def _():
            start_all(down_copies(layer + 1))

        wait_all(cache)
        for t in range(n_t):
            swap_b[t].wait()
            cols = slice(t * tw, (t + 1) * tw)
            res = (snd_b[t].astype(F32) + rcv_b[t].astype(F32)).astype(BF16)
            x_buf[:, cols] = (x_buf[:, cols].astype(F32) + res.astype(F32)).astype(BF16)
        return carry

    lax.fori_loop(0, n_layers, layer_step, 0)
    hid_out[...] = x_buf[mine, :]


def hand_over(a_ref, b_ref, c_ref, a_out, b_out, c_out):
    a_out[...] = a_ref[...]
    b_out[...] = b_ref[...]
    c_out[...] = c_ref[...]


def solution(mesh):
    tok_spec = P(('dp', 'sp', 'tp'))
    col_spec = P(None, None, 'tp')
    row_spec = P(None, 'tp', None)
    cache_spec = P(None, ('dp', 'sp'), 'tp', None)

    def device_fn(hidden_in, segment_ids, positions, attn_gain, w_q, w_k, w_v, w_o, mlp_gain, w_gate, w_up, w_down):
        half_rows, d_model = hidden_in.shape
        rows = 2 * half_rows
        n_layers, _, n_q = w_q.shape
        ffn = w_gate.shape[2]
        half_dim = HEAD_DIM // 2
        inv_freq = ROPE_BASE ** (-jnp.arange(half_dim, dtype=F32) / half_dim)
        angles = positions.astype(F32)[:, None] * inv_freq
        cos_val = jnp.cos(angles)
        sin_val = jnp.sin(angles)
        aux = jnp.stack([jnp.concatenate([cos_val, cos_val], axis=1), jnp.concatenate([-sin_val, sin_val], axis=1),
                         jnp.broadcast_to(segment_ids.astype(F32)[:, None], (half_rows, HEAD_DIM))])
        vm = pl.BlockSpec(memory_space=pltpu.VMEM)
        anyspec = pl.BlockSpec(memory_space=pl.ANY)
        n_t, tw = 3, d_model // 3
        dma = pltpu.SemaphoreType.DMA
        body = lambda *refs: stack_kernel(n_layers, rows, half_rows, *refs)
        hid, k_c, v_c = pl.pallas_call(
            body,
            out_shape=(jax.ShapeDtypeStruct((half_rows, d_model), BF16),
                       jax.ShapeDtypeStruct((n_layers, rows, HEAD_DIM), BF16),
                       jax.ShapeDtypeStruct((n_layers, rows, HEAD_DIM), BF16)),
            in_specs=[vm, vm, vm, vm] + [anyspec] * 7,
            out_specs=(vm, anyspec, anyspec),
            scratch_shapes=[
                pltpu.VMEM((rows, d_model), BF16),
                pltpu.VMEM((3, rows, 128), F32),
                pltpu.VMEM((4, 4, 4, 16, 128), F32),
                pltpu.VMEM((d_model, n_q + 2 * HEAD_DIM), BF16),
                pltpu.VMEM((n_q, d_model), BF16),
                pltpu.VMEM((d_model, ffn), BF16),
                pltpu.VMEM((d_model, ffn), BF16),
                pltpu.VMEM((ffn, d_model), BF16),
                *[pltpu.VMEM((2, RING, RING, RING, r, 2 * LANES), BF16) for r in PART_ROWS],
                *[pltpu.VMEM((RING, RING, RING, r, LANES), BF16) for r in PART_ROWS],
                pltpu.VMEM((256, n_q), BF16),
                pltpu.VMEM((rows, LANES), F32),
                pltpu.VMEM((8, n_q), F32),
                pltpu.VMEM((8, n_q), F32),
                pltpu.VMEM((HEAD_DIM, n_q), F32),
                pltpu.VMEM((rows, d_model), BF16),
                pltpu.VMEM((rows, n_q), BF16),
                pltpu.VMEM((rows, ffn), BF16),
                pltpu.VMEM((rows, HEAD_DIM), BF16),
                pltpu.VMEM((rows, HEAD_DIM), BF16),
                pltpu.VMEM((n_t, rows, tw), BF16),
                pltpu.VMEM((n_t, rows, tw), BF16),
                pltpu.VMEM((n_t, rows, tw), BF16),
                pltpu.VMEM((n_t, rows, tw), BF16),
                pltpu.VMEM((2, n_layers, d_model), F32),
                dma((2,)), dma((2,)), dma((9,)), dma((9,)), dma((16,)),
                dma((3, N_SEM)), dma((2, 3, N_SEM)), dma((2, n_t)), dma((2, n_t)), dma((2,)),
            ],
            compiler_params=pltpu.CompilerParams(collective_id=0, has_side_effects=True, vmem_limit_bytes=67043328),
        )(hidden_in, aux, attn_gain, mlp_gain, w_q, w_k, w_v, w_o, w_gate, w_up, w_down)
        hid, k_c, v_c = pl.pallas_call(
            hand_over, out_shape=tuple(jax.ShapeDtypeStruct(r.shape, r.dtype) for r in (hid, k_c, v_c)),
            in_specs=[vm] * 3, out_specs=(vm, vm, vm))(hid, k_c, v_c)
        return hid, k_c.reshape(n_layers, rows, 1, HEAD_DIM), v_c.reshape(n_layers, rows, 1, HEAD_DIM)

    return jax.shard_map(device_fn, mesh=mesh,
                         in_specs=(P(('dp', 'sp', 'tp'), None), tok_spec, tok_spec, P(), col_spec, col_spec, col_spec, row_spec, P(), col_spec, col_spec, row_spec),
                         out_specs=(P(('dp', 'sp', 'tp'), None), cache_spec, cache_spec), check_vma=False)
```
